32 devices in a mesh: gx: 4 (over z), gy: 2 (over x), gz: 4 (over y, core).
Axes of the slice: x: 2, y: 2, z: 4, core: 2. Of those that a mesh axis runs over, the one named last changes fastest.
Arguments:
- fields_now: float32 [24, 32, 16, 512], P(None, 'gx', 'gy', 'gz'), may hold values from -6 to 6
- parent: float32 [24, 32, 16, 512], P(None, 'gx', 'gy', 'gz'), may hold values from -6 to 6
- advect: float32 [3, 24, 24], replicated, may hold values from -0.75 to 0.75
- diffuse: float32 [3, 24, 24], replicated, may hold values from -0.25 to 0.25
- box_shift: int32 [3], replicated, may hold values from 1 to 4
Outputs:
- section_slope: float32 [24, 32, 16, 512], P(None, 'gx', 'gy', 'gz')
- section_value: float32 [24, 32, 16, 512], P(None, 'gx', 'gy', 'gz')
The draws below stay inside these ranges and needn't reach their ends.
All inputs are finite; a program needn't handle non-finite values.
Results may differ from the reference program's by a relative error of at most 0.0001.
Values sent between devices are 32-bit elements; how exact they have to be, the bound alone decides.
A program may use at most 64 MiB of HBM per device.

```python
import jax
import jax.numpy as jnp
from jax import lax

F = 24
NX = 32
NY = 16
NZ = 512


def level_of(rng, shape, shards, low, top_value):
    gain, own = 1.0, jax.random.fold_in(rng, 6)
    for dim, parts in shards:
        heights = jnp.exp(jax.random.uniform(jax.random.fold_in(own, dim), (parts,), jnp.float32, low / len(shards), top_value / len(shards)))
        gain = gain * jnp.repeat(heights, shape[dim] // parts).reshape([-1 if axis == dim else 1 for axis in range(len(shape))])
    return gain


def scatter_about(own_key, shape, width, most, pieces=(), held_as=jnp.bfloat16):
    values = width * jax.random.normal(own_key, shape, jnp.float32)
    if pieces:
        values = values * level_of(own_key, shape, pieces, -0.22, 0.18)
    return jnp.clip(values, -most, most).astype(held_as)


def setup_inputs(seed: int = 0) -> dict:
    keys = jax.random.split(jax.random.key(seed), 6)
    fields_now = scatter_about(keys[0], (F, NX, NY, NZ), 1.0, 6.0, ((1, 4), (2, 2), (3, 4)), jnp.float32)
    parent = scatter_about(keys[1], (F, NX, NY, NZ), 1.0, 6.0, ((1, 4), (2, 2), (3, 4)), jnp.float32)
    advect = scatter_about(keys[2], (3, F, F), (3 * F) ** -0.5, 0.75, (), jnp.float32)
    diffuse = scatter_about(keys[3], (3, F, F), (27 * F) ** -0.5, 0.25, (), jnp.float32)
    box_shift = jax.random.randint(keys[4], (3,), 1, 5).astype(jnp.int32)
    return {"fields_now": fields_now, "parent": parent, "advect": advect, "diffuse": diffuse, "box_shift": box_shift}


dissipation = 1.0
half_step = 0.125


def line_terms(padded_line, axis):
    length = padded_line.shape[axis] - 6

    def take_at(offset):
        return lax.slice_in_dim(padded_line, 3 + offset, 3 + offset + length, axis=axis)

    first_diff = (take_at(-2) - 8.0 * take_at(-1) + 8.0 * take_at(1) - take_at(2)) / 12.0
    second_diff = (-take_at(-2) + 16.0 * take_at(-1) - 30.0 * take_at(0) + 16.0 * take_at(1) - take_at(2)) / 12.0
    sixth_diff = (take_at(-3) - 6.0 * take_at(-2) + 15.0 * take_at(-1) - 20.0 * take_at(0)
                  + 15.0 * take_at(1) - 6.0 * take_at(2) + take_at(3))
    return first_diff, second_diff, sixth_diff


def mix_fields(matrix, field):
    flat = field.reshape(field.shape[0], -1)
    return jnp.dot(matrix, flat, precision=lax.Precision.HIGHEST,
                   preferred_element_type=jnp.float32).reshape(field.shape)


def center_crop(padded, axis):
    window = [slice(None)] * 4
    for other in (1, 2, 3):
        if other != axis:
            window[other] = slice(3, padded.shape[other] - 3)
    return padded[tuple(window)]


def axis_terms(line, axis, advect, diffuse):
    first_diff, second_diff, sixth_diff = line_terms(line, axis)
    coupled = mix_fields(advect[axis - 1], first_diff) + mix_fields(diffuse[axis - 1], second_diff)
    return coupled, sixth_diff


def whole_terms(padded, advect, diffuse):
    linear, smooth = axis_terms(center_crop(padded, 1), 1, advect, diffuse)
    for axis in (2, 3):
        coupled, sixth_diff = axis_terms(center_crop(padded, axis), axis, advect, diffuse)
        linear = linear + coupled
        smooth = smooth + sixth_diff
    return linear, smooth


def finish(new_box, linear, smooth):
    lapse_factor = 1.0 + 0.25 * jnp.tanh(new_box[0])
    section_slope = lapse_factor * linear + (dissipation / 64.0) * smooth
    section_value = new_box + half_step * section_slope
    return section_slope, section_value


def reference(fields_now, parent, advect, diffuse, box_shift):
    room = jnp.pad(fields_now, ((0, 0), (0, 4), (0, 4), (0, 4)))
    anchor = jnp.zeros((), jnp.int32)
    moved_cells = lax.dynamic_slice(room, (anchor, box_shift[0], box_shift[1], box_shift[2]), fields_now.shape)
    keep_mask = None
    for axis in (1, 2, 3):
        shape_one = [1, 1, 1, 1]
        shape_one[axis] = fields_now.shape[axis]
        position = lax.broadcasted_iota(jnp.int32, tuple(shape_one), axis)
        inside = position + box_shift[axis - 1] < fields_now.shape[axis]
        keep_mask = inside if keep_mask is None else keep_mask & inside
    new_box = jnp.where(keep_mask, moved_cells, parent)
    padded = jnp.pad(new_box, ((0, 0), (3, 3), (3, 3), (3, 3)))
    linear, smooth = whole_terms(padded, advect, diffuse)
    return finish(new_box, linear, smooth)
```

```python
import functools

import jax
import jax.numpy as jnp
from jax import lax
from jax.experimental import pallas as pl
from jax.experimental.pallas import tpu as pltpu
from jax.sharding import PartitionSpec as P

MESH = pl.DeviceIdType.MESH
W = 4
H = 3
SLOT = 8
AXES = ("gx", "gy", "gz")


def roll(value, by):
    return pltpu.roll(value, by % value.shape[-1], value.ndim - 1)


def kernel(
    dims, shift_ref, now_ref, parent_ref, advect_ref, diffuse_ref, slope_ref, value_ref,
    old, box, edge, edge_in, rim, rim_up, rim_low, send_sem, recv_sem,
):
    F, NX, NY, NZ = dims
    cells = NX * NY
    slots = NZ // SLOT
    groups = cells // slots
    me = {a: lax.axis_index(a) for a in AXES}
    size = {a: lax.axis_size(a) for a in AXES}
    below = {a: me[a] > 0 for a in AXES}
    above = {a: me[a] < size[a] - 1 for a in AXES}
    move = [shift_ref[d] for d in range(3)]

    class Copy:
        def __init__(self, n, src, dst, axis, by):
            self.sends = below[axis] if by < 0 else above[axis]
            self.gets = above[axis] if by < 0 else below[axis]
            self.copy = pltpu.make_async_remote_copy(
                src_ref=src, dst_ref=dst, send_sem=send_sem.at[n], recv_sem=recv_sem.at[n],
                device_id={axis: me[axis] + by}, device_id_type=MESH,
            )

        def start(self):
            pl.when(self.sends)(self.copy.start)

        def arrived(self):
            pl.when(self.gets)(self.copy.wait_recv)

        def sent(self):
            pl.when(self.sends)(self.copy.wait_send)

    rim_up[...] = jnp.zeros_like(rim_up)
    rim_low[...] = jnp.zeros_like(rim_low)
    blank = jnp.zeros((F, NZ), jnp.float32)

    def clear_x(y, _):
        for x in (*range(H), *range(NX + H, NX + 2 * H)):
            box[x, y + H] = blank
        return 0

    def clear_y(x, _):
        for y in (*range(H), *range(NY + H, NY + 2 * H)):
            box[x + H, y] = blank
        return 0

    lax.fori_loop(0, NY, clear_x, 0)
    lax.fori_loop(0, NX, clear_y, 0)

    barrier = pltpu.get_barrier_semaphore()
    count = 0
    for a in AXES:
        for cond, by in ((below[a], -1), (above[a], 1)):
            @pl.when(cond)
            def _(a=a, by=by):
                pl.semaphore_signal(
                    barrier, inc=1, device_id={a: me[a] + by}, device_id_type=MESH
                )
        count = count + jnp.where(me[a] > 0, 1, 0) + jnp.where(me[a] < size[a] - 1, 1, 0)

    lane = lax.broadcasted_iota(jnp.int32, (F, NZ), 1)
    slot_of = ((lane + SLOT // 2) % NZ) // SLOT

    def place(g, j):
        k = g * slots + j
        return k, g * (slots // NY) + j // NY, j % NY

    def pack_old(g, _):
        packed = blank
        for j in range(slots):
            k, _, _ = place(g, j)
            row = now_ref[pl.ds(k, F, stride=cells), :]
            packed = jnp.where(slot_of == j, roll(row, SLOT * j), packed)
        edge[g] = packed
        return 0

    lax.fori_loop(0, groups, pack_old, 0)
    pl.semaphore_wait(barrier, count)

    c_edge = Copy(0, edge, edge_in, "gz", -1)
    c_edge.start()
    c_edge.arrived()

    def move_z(g, _):
        for j in range(slots):
            k, x, y = place(g, j)
            row = now_ref[pl.ds(k, F, stride=cells), :]
            tail = roll(edge_in[g], -SLOT * j)
            old[x, y] = pltpu.roll(jnp.where(lane < move[2], tail, row), NZ - move[2], 1)
        return 0

    lax.fori_loop(0, groups, move_z, 0)

    X, Y = pl.ds(0, NX), pl.ds(0, NY)
    half = W // 2
    c_x = Copy(1, old.at[pl.ds(0, W), Y], old.at[pl.ds(NX, W), Y], "gx", -1)
    c_y = Copy(2, old.at[X, pl.ds(0, W)], old.at[X, pl.ds(NY, W)], "gy", -1)
    c_x.start()
    c_y.start()
    c_x.arrived()
    c_cy = Copy(
        3, old.at[pl.ds(NX, half), pl.ds(0, W)], old.at[pl.ds(NX, half), pl.ds(NY, W)], "gy", -1
    )
    c_cy.start()
    c_y.arrived()
    c_cx = Copy(
        4, old.at[pl.ds(half, half), pl.ds(NY, W)],
        old.at[pl.ds(NX + half, half), pl.ds(NY, W)], "gx", -1,
    )
    c_cx.start()
    c_cy.arrived()
    c_cx.arrived()

    in_z = me["gz"] * NZ + lane + move[2] < size["gz"] * NZ

    def move_xy(g, _):
        packed = blank
        for j in range(slots):
            k, x, y = place(g, j)
            in_x = me["gx"] * NX + x + move[0] < size["gx"] * NX
            in_y = me["gy"] * NY + y + move[1] < size["gy"] * NY
            inside = in_z & (in_x & in_y)
            row = jnp.where(
                inside, old[x + move[0], y + move[1]], parent_ref[pl.ds(k, F, stride=cells), :]
            )
            box[x + H, y + H] = row
            packed = jnp.where(slot_of == j, roll(row, SLOT * j), packed)
        rim[g] = packed
        return 0

    lax.fori_loop(0, groups, move_xy, 0)

    BX, BY = pl.ds(H, NX), pl.ds(H, NY)
    halos = [
        Copy(5, box.at[pl.ds(H, H), BY], box.at[pl.ds(NX + H, H), BY], "gx", -1),
        Copy(6, box.at[pl.ds(NX, H), BY], box.at[pl.ds(0, H), BY], "gx", 1),
        Copy(7, box.at[BX, pl.ds(H, H)], box.at[BX, pl.ds(NY + H, H)], "gy", -1),
        Copy(8, box.at[BX, pl.ds(NY, H)], box.at[BX, pl.ds(0, H)], "gy", 1),
        Copy(9, rim, rim_up, "gz", -1),
        Copy(10, rim, rim_low, "gz", 1),
    ]
    for c in halos:
        c.start()
    mats = []
    for a in range(3):
        mats += [advect_ref[a], diffuse_ref[a]]
    matrix = jnp.concatenate(mats, axis=1) / 12.0
    m_high = matrix.astype(jnp.bfloat16)
    m_low = (matrix - m_high.astype(jnp.float32)).astype(jnp.bfloat16)
    for c in halos:
        c.arrived()

    def terms(u, at):
        d1, s1 = at(1) - at(-1), at(1) + at(-1)
        d2, s2 = at(2) - at(-2), at(2) + at(-2)
        s3 = at(3) + at(-3)
        first = 8.0 * d1 - d2
        second = 16.0 * s1 - 30.0 * u - s2
        sixth = s3 - 6.0 * s2 + 15.0 * s1 - 20.0 * u
        return first, second, sixth

    def compute(g, _):
        rims = jnp.where(lane % SLOT < SLOT // 2, rim_up[g], rim_low[g])
        for j0 in range(0, slots, 2):
            columns, us, smooths, ks = [], [], [], []
            for j in (j0, j0 + 1):
                k, x, y = place(g, j)
                u = box[x + H, y + H]
                ends = roll(rims, -SLOT * j)
                z_at = {}
                for o in range(1, H + 1):
                    z_at[o] = roll(jnp.where(lane < o, ends, u), -o)
                    z_at[-o] = roll(jnp.where(lane >= NZ - o, ends, u), o)
                fx, sx, x6 = terms(u, lambda o: box[x + H + o, y + H])
                fy, sy, y6 = terms(u, lambda o: box[x + H, y + H + o])
                fz, sz, z6 = terms(u, lambda o: z_at[o])
                columns.append(jnp.concatenate([fx, sx, fy, sy, fz, sz], axis=0))
                us.append(u)
                smooths.append(x6 + y6 + z6)
                ks.append(k)
            column = jnp.concatenate(columns, axis=1)
            high = column.astype(jnp.bfloat16)
            low = (column - high.astype(jnp.float32)).astype(jnp.bfloat16)
            dot = functools.partial(jnp.dot, preferred_element_type=jnp.float32)
            linear = dot(m_high, high) + (dot(m_low, high) + dot(m_high, low))
            for i in range(2):
                lapse = 1.0 + 0.25 * jnp.tanh(us[i][0:1, :])
                slope = lapse * linear[:, i * NZ:(i + 1) * NZ] + smooths[i] * (1.0 / 64.0)
                slope_ref[pl.ds(ks[i], F, stride=cells), :] = slope
                value_ref[pl.ds(ks[i], F, stride=cells), :] = us[i] + 0.125 * slope
        return 0

    lax.fori_loop(0, groups, compute, 0)

    for c in [c_edge, c_x, c_y, c_cy, c_cx] + halos:
        c.sent()


def local(fields_now, parent, advect, diffuse, box_shift):
    dims = fields_now.shape
    F, NX, NY, NZ = dims
    flat = (F * NX * NY, NZ)
    groups = NX * NY * SLOT // NZ
    edges = pltpu.VMEM((groups, F, NZ), jnp.float32)
    vmem = pl.BlockSpec(memory_space=pltpu.VMEM)
    slope, value = pl.pallas_call(
        functools.partial(kernel, dims),
        out_shape=[jax.ShapeDtypeStruct(flat, jnp.float32)] * 2,
        in_specs=[pl.BlockSpec(memory_space=pltpu.SMEM)] + [vmem] * 4,
        out_specs=[vmem] * 2,
        scratch_shapes=[
            pltpu.VMEM((NX + W, NY + W, F, NZ), jnp.float32),
            pltpu.VMEM((NX + 2 * H, NY + 2 * H, F, NZ), jnp.float32),
            edges, edges, edges, edges, edges,
            pltpu.SemaphoreType.DMA((11,)),
            pltpu.SemaphoreType.DMA((11,)),
        ],
        compiler_params=pltpu.CompilerParams(collective_id=0, has_side_effects=True),
    )(box_shift, fields_now.reshape(flat), parent.reshape(flat), advect, diffuse)
    return slope.reshape(dims), value.reshape(dims)


def solution(mesh):
    return jax.shard_map(
        local,
        mesh=mesh,
        in_specs=(P(None, "gx", "gy", "gz"), P(None, "gx", "gy", "gz"), P(), P(), P()),
        out_specs=(P(None, "gx", "gy", "gz"), P(None, "gx", "gy", "gz")),
        check_vma=False,
    )
```

```python
import functools

import jax
import jax.numpy as jnp
from jax import lax
from jax.experimental import pallas as pl
from jax.experimental.pallas import tpu as pltpu
from jax.sharding import PartitionSpec as P

MESH = pl.DeviceIdType.MESH
W = 4
H = 3
SLOT = 8
ROWS = 8
AXES = ("gx", "gy", "gz")


def roll(value, by):
    return pltpu.roll(value, by % value.shape[-1], value.ndim - 1)


def kernel(
    dims, shift_ref, now_hbm, parent_hbm, advect_ref, diffuse_ref, slope_ref, value_ref,
    now_ref, parent_ref, box, edge, edge_in, rim, rim_up, rim_low, mixed, smooth_ref,
    send_sem, recv_sem, load_sem, *old,
):
    F, NX, NY, NZ = dims
    chunks = F // ROWS
    cells = NX * NY
    slots = NZ // SLOT
    groups = cells // slots
    me = {a: lax.axis_index(a) for a in AXES}
    size = {a: lax.axis_size(a) for a in AXES}
    below = {a: me[a] > 0 for a in AXES}
    above = {a: me[a] < size[a] - 1 for a in AXES}
    move = [shift_ref[d] for d in range(3)]
    sems = iter(range(1 + 10 * chunks))

    load_now = pltpu.make_async_copy(now_hbm, now_ref, load_sem.at[0])
    load_parent = pltpu.make_async_copy(parent_hbm, parent_ref, load_sem.at[1])
    load_now.start()
    load_parent.start()

    class Copy:
        def __init__(self, src, dst, axis, by):
            n = next(sems)
            self.sends = below[axis] if by < 0 else above[axis]
            self.gets = above[axis] if by < 0 else below[axis]
            self.copy = pltpu.make_async_remote_copy(
                src_ref=src, dst_ref=dst, send_sem=send_sem.at[n], recv_sem=recv_sem.at[n],
                device_id={axis: me[axis] + by}, device_id_type=MESH,
            )

        def start(self):
            pl.when(self.sends)(self.copy.start)

        def arrived(self):
            pl.when(self.gets)(self.copy.wait_recv)

        def sent(self):
            pl.when(self.sends)(self.copy.wait_send)

    rim_up[...] = jnp.zeros_like(rim_up)
    rim_low[...] = jnp.zeros_like(rim_low)
    blank = jnp.zeros((ROWS, NZ), jnp.float32)

    def clear_x(y, _):
        for c in range(chunks):
            for x in (*range(H), *range(NX + H, NX + 2 * H)):
                box[c, x, y + H] = blank
        return 0

    def clear_y(x, _):
        for c in range(chunks):
            for y in (*range(H), *range(NY + H, NY + 2 * H)):
                box[c, x + H, y] = blank
        return 0

    lax.fori_loop(0, NY, clear_x, 0)
    lax.fori_loop(0, NX, clear_y, 0)

    barrier = pltpu.get_barrier_semaphore()
    count = 0
    for a in AXES:
        for cond, by in ((below[a], -1), (above[a], 1)):
            @pl.when(cond)
            def _(a=a, by=by):
                pl.semaphore_signal(
                    barrier, inc=1, device_id={a: me[a] + by}, device_id_type=MESH
                )
        count = count + jnp.where(me[a] > 0, 1, 0) + jnp.where(me[a] < size[a] - 1, 1, 0)

    lane = lax.broadcasted_iota(jnp.int32, (ROWS, NZ), 1)
    slot_of = ((lane + SLOT // 2) % NZ) // SLOT

    def place(g, j):
        k = g * slots + j
        return k, g * (slots // NY) + j // NY, j % NY

    def rows_of(c, k):
        return pl.ds(c * ROWS * cells + k, ROWS, stride=cells)

    load_now.wait()

    def pack_old(g, _):
        for c in range(chunks):
            packed = blank
            for j in range(slots):
                k, _, _ = place(g, j)
                packed = jnp.where(slot_of == j, roll(now_ref[rows_of(c, k), :], SLOT * j), packed)
            edge[c, g] = packed
        return 0

    lax.fori_loop(0, groups, pack_old, 0)
    pl.semaphore_wait(barrier, count)

    c_edge = Copy(edge, edge_in, "gz", -1)
    c_edge.start()

    X, Y = pl.ds(0, NX), pl.ds(0, NY)
    BX, BY = pl.ds(H, NX), pl.ds(H, NY)
    half = W // 2
    near, far = pl.ds(NX, half), pl.ds(NX + half, half)
    to_x, to_y, corner_y, corner_x, halos = [], [], [], [], []
    for c in range(chunks):
        o, b = old[c], box.at[c]
        to_x.append(Copy(o.at[pl.ds(0, W), Y], o.at[pl.ds(NX, W), Y], "gx", -1))
        to_y.append(Copy(o.at[X, pl.ds(0, W)], o.at[X, pl.ds(NY, W)], "gy", -1))
        corner_y.append(Copy(o.at[near, pl.ds(0, W)], o.at[near, pl.ds(NY, W)], "gy", -1))
        corner_x.append(
            Copy(o.at[pl.ds(half, half), pl.ds(NY, W)], o.at[far, pl.ds(NY, W)], "gx", -1)
        )
        halos.append([
            Copy(b.at[pl.ds(H, H), BY], b.at[pl.ds(NX + H, H), BY], "gx", -1),
            Copy(b.at[pl.ds(NX, H), BY], b.at[pl.ds(0, H), BY], "gx", 1),
            Copy(b.at[BX, pl.ds(H, H)], b.at[BX, pl.ds(NY + H, H)], "gy", -1),
            Copy(b.at[BX, pl.ds(NY, H)], b.at[BX, pl.ds(0, H)], "gy", 1),
            Copy(rim.at[c], rim_up.at[c], "gz", -1),
            Copy(rim.at[c], rim_low.at[c], "gz", 1),
        ])

    def move_z(c):
        def step(g, _):
            for j in range(slots):
                k, x, y = place(g, j)
                tail = roll(edge_in[c, g], -SLOT * j)
                row = jnp.where(lane < move[2], tail, now_ref[rows_of(c, k), :])
                old[c][x, y] = pltpu.roll(row, NZ - move[2], 1)
            return 0

        lax.fori_loop(0, groups, step, 0)

    def send_old(c):
        to_x[c].start()
        to_y[c].start()

    def send_corner(c):
        to_x[c].arrived()
        corner_y[c].start()
        to_y[c].arrived()
        corner_x[c].start()

    in_z = me["gz"] * NZ + lane + move[2] < size["gz"] * NZ

    def move_xy(c):
        corner_y[c].arrived()
        corner_x[c].arrived()

        def step(g, _):
            packed = blank
            for j in range(slots):
                k, x, y = place(g, j)
                in_x = me["gx"] * NX + x + move[0] < size["gx"] * NX
                in_y = me["gy"] * NY + y + move[1] < size["gy"] * NY
                row = jnp.where(
                    in_z & (in_x & in_y),
                    old[c][x + move[0], y + move[1]],
                    parent_ref[rows_of(c, k), :],
                )
                box[c, x + H, y + H] = row
                packed = jnp.where(slot_of == j, roll(row, SLOT * j), packed)
            rim[c, g] = packed
            return 0

        lax.fori_loop(0, groups, step, 0)
        for h in halos[c]:
            h.start()

    def split(value):
        high = value.astype(jnp.bfloat16)
        return high, (value - high.astype(jnp.float32)).astype(jnp.bfloat16)

    def terms(u, at):
        d1, s1 = at(1) - at(-1), at(1) + at(-1)
        d2, s2 = at(2) - at(-2), at(2) + at(-2)
        s3 = at(3) + at(-3)
        first = 8.0 * d1 - d2
        second = 16.0 * s1 - 30.0 * u - s2
        sixth = s3 - 6.0 * s2 + 15.0 * s1 - 20.0 * u
        return first, second, sixth

    def compute(c):
        for h in halos[c]:
            h.arrived()
        fields = slice(c * ROWS, (c + 1) * ROWS)
        mats = [m[a][:, fields] for a in range(3) for m in (advect_ref, diffuse_ref)]
        m_high, m_low = split(jnp.concatenate(mats, axis=1) / 12.0)
        dot = functools.partial(jnp.dot, preferred_element_type=jnp.float32)

        def step(g, _):
            rims = jnp.where(lane % SLOT < SLOT // 2, rim_up[c, g], rim_low[c, g])
            for j0 in range(0, slots, 2):
                columns = []
                for j in (j0, j0 + 1):
                    k, x, y = place(g, j)
                    u = box[c, x + H, y + H]
                    ends = roll(rims, -SLOT * j)
                    z_at = {}
                    for o in range(1, H + 1):
                        z_at[o] = roll(jnp.where(lane < o, ends, u), -o)
                        z_at[-o] = roll(jnp.where(lane >= NZ - o, ends, u), o)
                    fx, sx, x6 = terms(u, lambda o: box[c, x + H + o, y + H])
                    fy, sy, y6 = terms(u, lambda o: box[c, x + H, y + H + o])
                    fz, sz, z6 = terms(u, lambda o: z_at[o])
                    columns.append(jnp.concatenate([fx, sx, fy, sy, fz, sz], axis=0))
                    smooth_ref[c, k] = (x6 + y6 + z6) * (1.0 / 64.0)
                high, low = split(jnp.concatenate(columns, axis=1))
                linear = dot(m_high, high) + (dot(m_low, high) + dot(m_high, low))
                for i in range(2):
                    k = g * slots + j0 + i
                    part = linear[:, i * NZ:(i + 1) * NZ]
                    if c > 0:
                        part = part + mixed[k]
                    if c < chunks - 1:
                        mixed[k] = part
                        continue
                    _, x, y = place(g, j0 + i)
                    lapse = 1.0 + 0.25 * jnp.tanh(box[0, x + H, y + H][0:1, :])
                    for n in range(chunks):
                        slope = lapse * part[n * ROWS:(n + 1) * ROWS] + smooth_ref[n, k]
                        slope_ref[rows_of(n, k), :] = slope
                        value_ref[rows_of(n, k), :] = box[n, x + H, y + H] + 0.125 * slope
            return 0

        lax.fori_loop(0, groups, step, 0)

    c_edge.arrived()
    move_z(0)
    send_old(0)
    for c in range(1, chunks):
        move_z(c)
    load_parent.wait()
    for c in range(chunks):
        if c + 1 < chunks:
            to_x[c].sent()
            to_y[c].sent()
            send_old(c + 1)
        send_corner(c)
        if c > 1:
            compute(c - 2)
        move_xy(c)
    for c in range(max(chunks - 2, 0), chunks):
        compute(c)

    c_edge.sent()
    to_x[-1].sent()
    to_y[-1].sent()
    for c in range(chunks):
        corner_y[c].sent()
        corner_x[c].sent()
        for h in halos[c]:
            h.sent()


def local(fields_now, parent, advect, diffuse, box_shift):
    dims = fields_now.shape
    F, NX, NY, NZ = dims
    flat = (F * NX * NY, NZ)
    chunks = F // ROWS
    groups = NX * NY * SLOT // NZ
    f32 = jnp.float32
    edges = pltpu.VMEM((chunks, groups, ROWS, NZ), f32)
    vmem = pl.BlockSpec(memory_space=pltpu.VMEM)
    hbm = pl.BlockSpec(memory_space=pl.ANY)
    slope, value = pl.pallas_call(
        functools.partial(kernel, dims),
        out_shape=[jax.ShapeDtypeStruct(flat, f32)] * 2,
        in_specs=[pl.BlockSpec(memory_space=pltpu.SMEM), hbm, hbm, vmem, vmem],
        out_specs=[vmem] * 2,
        scratch_shapes=[
            pltpu.VMEM(flat, f32),
            pltpu.VMEM(flat, f32),
            pltpu.VMEM((chunks, NX + 2 * H, NY + 2 * H, ROWS, NZ), f32),
            edges, edges, edges, edges, edges,
            pltpu.VMEM((NX * NY, F, NZ), f32),
            pltpu.VMEM((chunks, NX * NY, ROWS, NZ), f32),
            pltpu.SemaphoreType.DMA((1 + 10 * chunks,)),
            pltpu.SemaphoreType.DMA((1 + 10 * chunks,)),
            pltpu.SemaphoreType.DMA((2,)),
        ] + [pltpu.VMEM((NX + W, NY + W, ROWS, NZ), f32)] * chunks,
        compiler_params=pltpu.CompilerParams(collective_id=0, has_side_effects=True),
    )(box_shift, fields_now.reshape(flat), parent.reshape(flat), advect, diffuse)
    return slope.reshape(dims), value.reshape(dims)


def solution(mesh):
    return jax.shard_map(
        local,
        mesh=mesh,
        in_specs=(P(None, "gx", "gy", "gz"), P(None, "gx", "gy", "gz"), P(), P(), P()),
        out_specs=(P(None, "gx", "gy", "gz"), P(None, "gx", "gy", "gz")),
        check_vma=False,
    )
```

```python
import functools

import jax
import jax.numpy as jnp
from jax import lax
from jax.experimental import pallas as pl
from jax.experimental.pallas import tpu as pltpu
from jax.sharding import PartitionSpec as P

MESH = pl.DeviceIdType.MESH
W = 4
H = 3
SLOT = 8
ROWS = 8
AXES = ("gx", "gy", "gz")


def roll(value, by):
    return pltpu.roll(value, by % value.shape[-1], value.ndim - 1)


def kernel(
    dims, shift_ref, now_ref, parent_ref, advect_ref, diffuse_ref, slope_ref, value_ref,
    box, edge, edge_in, rim, rim_up, rim_low, mixed, smooth_ref,
    send_sem, recv_sem, *old,
):
    F, NX, NY, NZ = dims
    chunks = F // ROWS
    cells = NX * NY
    slots = NZ // SLOT
    groups = cells // slots
    me = {a: lax.axis_index(a) for a in AXES}
    size = {a: lax.axis_size(a) for a in AXES}
    below = {a: me[a] > 0 for a in AXES}
    above = {a: me[a] < size[a] - 1 for a in AXES}
    move = [shift_ref[d] for d in range(3)]
    sems = iter(range(11 * chunks))

    class Copy:
        def __init__(self, src, dst, axis, by):
            n = next(sems)
            self.sends = below[axis] if by < 0 else above[axis]
            self.gets = above[axis] if by < 0 else below[axis]
            self.copy = pltpu.make_async_remote_copy(
                src_ref=src, dst_ref=dst, send_sem=send_sem.at[n], recv_sem=recv_sem.at[n],
                device_id={axis: me[axis] + by}, device_id_type=MESH,
            )

        def start(self):
            pl.when(self.sends)(self.copy.start)

        def arrived(self):
            pl.when(self.gets)(self.copy.wait_recv)

        def sent(self):
            pl.when(self.sends)(self.copy.wait_send)

    rim_up[...] = jnp.zeros_like(rim_up)
    rim_low[...] = jnp.zeros_like(rim_low)
    blank = jnp.zeros((ROWS, NZ), jnp.float32)

    def clear_x(y, _):
        for c in range(chunks):
            for x in (*range(H), *range(NX + H, NX + 2 * H)):
                box[c, x, y + H] = blank
        return 0

    def clear_y(x, _):
        for c in range(chunks):
            for y in (*range(H), *range(NY + H, NY + 2 * H)):
                box[c, x + H, y] = blank
        return 0

    lax.fori_loop(0, NY, clear_x, 0)
    lax.fori_loop(0, NX, clear_y, 0)

    barrier = pltpu.get_barrier_semaphore()
    count = 0
    for a in AXES:
        for cond, by in ((below[a], -1), (above[a], 1)):
            @pl.when(cond)
            def _(a=a, by=by):
                pl.semaphore_signal(
                    barrier, inc=1, device_id={a: me[a] + by}, device_id_type=MESH
                )
        count = count + jnp.where(me[a] > 0, 1, 0) + jnp.where(me[a] < size[a] - 1, 1, 0)

    lane = lax.broadcasted_iota(jnp.int32, (ROWS, NZ), 1)
    slot_of = ((lane + SLOT // 2) % NZ) // SLOT

    def place(g, j):
        k = g * slots + j
        return k, g * (slots // NY) + j // NY, j % NY

    def rows_of(c, k):
        return pl.ds(c * ROWS * cells + k, ROWS, stride=cells)

    def pack_old(c):
        def step(g, _):
            packed = blank
            for j in range(slots):
                k, _, _ = place(g, j)
                packed = jnp.where(slot_of == j, roll(now_ref[rows_of(c, k), :], SLOT * j), packed)
            edge[c, g] = packed
            return 0

        lax.fori_loop(0, groups, step, 0)

    edges = [Copy(edge.at[c], edge_in.at[c], "gz", -1) for c in range(chunks)]
    for c in range(chunks):
        pack_old(c)
        if c == 0:
            pl.semaphore_wait(barrier, count)
        edges[c].start()

    X, Y = pl.ds(0, NX), pl.ds(0, NY)
    BX, BY = pl.ds(H, NX), pl.ds(H, NY)
    half = W // 2
    near, far = pl.ds(NX, half), pl.ds(NX + half, half)
    to_x, to_y, corner_y, corner_x, halos = [], [], [], [], []
    for c in range(chunks):
        o, b = old[c], box.at[c]
        to_x.append(Copy(o.at[pl.ds(0, W), Y], o.at[pl.ds(NX, W), Y], "gx", -1))
        to_y.append(Copy(o.at[X, pl.ds(0, W)], o.at[X, pl.ds(NY, W)], "gy", -1))
        corner_y.append(Copy(o.at[near, pl.ds(0, W)], o.at[near, pl.ds(NY, W)], "gy", -1))
        corner_x.append(
            Copy(o.at[pl.ds(half, half), pl.ds(NY, W)], o.at[far, pl.ds(NY, W)], "gx", -1)
        )
        halos.append([
            Copy(b.at[pl.ds(H, H), BY], b.at[pl.ds(NX + H, H), BY], "gx", -1),
            Copy(b.at[pl.ds(NX, H), BY], b.at[pl.ds(0, H), BY], "gx", 1),
            Copy(b.at[BX, pl.ds(H, H)], b.at[BX, pl.ds(NY + H, H)], "gy", -1),
            Copy(b.at[BX, pl.ds(NY, H)], b.at[BX, pl.ds(0, H)], "gy", 1),
            Copy(rim.at[c], rim_up.at[c], "gz", -1),
            Copy(rim.at[c], rim_low.at[c], "gz", 1),
        ])

    def move_z(c):
        edges[c].arrived()

        def step(g, _):
            for j in range(slots):
                k, x, y = place(g, j)
                tail = roll(edge_in[c, g], -SLOT * j)
                row = jnp.where(lane < move[2], tail, now_ref[rows_of(c, k), :])
                old[c][x, y] = pltpu.roll(row, NZ - move[2], 1)
            return 0

        lax.fori_loop(0, groups, step, 0)

    def send_old(c):
        to_x[c].start()
        to_y[c].start()

    def send_corner(c):
        to_x[c].arrived()
        corner_y[c].start()
        to_y[c].arrived()
        corner_x[c].start()

    def send_halos(c, down):
        for n, h in enumerate(halos[c]):
            if (n in (0, 2)) == down:
                h.start()

    in_z = me["gz"] * NZ + lane + move[2] < size["gz"] * NZ

    def move_xy(c):
        corner_y[c].arrived()
        corner_x[c].arrived()

        def step(g, _):
            packed = blank
            for j in range(slots):
                k, x, y = place(g, j)
                in_x = me["gx"] * NX + x + move[0] < size["gx"] * NX
                in_y = me["gy"] * NY + y + move[1] < size["gy"] * NY
                row = jnp.where(
                    in_z & (in_x & in_y),
                    old[c][x + move[0], y + move[1]],
                    parent_ref[rows_of(c, k), :],
                )
                box[c, x + H, y + H] = row
                packed = jnp.where(slot_of == j, roll(row, SLOT * j), packed)
            rim[c, g] = packed
            return 0

        lax.fori_loop(0, groups, step, 0)
        send_halos(c, False)

    def split(value):
        high = value.astype(jnp.bfloat16)
        return high, (value - high.astype(jnp.float32)).astype(jnp.bfloat16)

    def terms(u, at):
        d1, s1 = at(1) - at(-1), at(1) + at(-1)
        d2, s2 = at(2) - at(-2), at(2) + at(-2)
        s3 = at(3) + at(-3)
        first = 8.0 * d1 - d2
        second = 16.0 * s1 - 30.0 * u - s2
        sixth = s3 - 6.0 * s2 + 15.0 * s1 - 20.0 * u
        return first, second, sixth

    def compute(c):
        for h in halos[c]:
            h.arrived()
        fields = slice(c * ROWS, (c + 1) * ROWS)
        mats = [m[a][:, fields] for a in range(3) for m in (advect_ref, diffuse_ref)]
        m_high, m_low = split(jnp.concatenate(mats, axis=1) / 12.0)
        dot = functools.partial(jnp.dot, preferred_element_type=jnp.float32)

        def step(g, _):
            rims = jnp.where(lane % SLOT < SLOT // 2, rim_up[c, g], rim_low[c, g])
            for j0 in range(0, slots, 2):
                columns = []
                for j in (j0, j0 + 1):
                    k, x, y = place(g, j)
                    u = box[c, x + H, y + H]
                    ends = roll(rims, -SLOT * j)
                    z_at = {}
                    for o in range(1, H + 1):
                        z_at[o] = roll(jnp.where(lane < o, ends, u), -o)
                        z_at[-o] = roll(jnp.where(lane >= NZ - o, ends, u), o)
                    fx, sx, x6 = terms(u, lambda o: box[c, x + H + o, y + H])
                    fy, sy, y6 = terms(u, lambda o: box[c, x + H, y + H + o])
                    fz, sz, z6 = terms(u, lambda o: z_at[o])
                    columns.append(jnp.concatenate([fx, sx, fy, sy, fz, sz], axis=0))
                    smooth_ref[c, k] = (x6 + y6 + z6) * (1.0 / 64.0)
                high, low = split(jnp.concatenate(columns, axis=1))
                linear = dot(m_high, high) + (dot(m_low, high) + dot(m_high, low))
                for i in range(2):
                    k = g * slots + j0 + i
                    part = linear[:, i * NZ:(i + 1) * NZ]
                    if c > 0:
                        part = part + mixed[k]
                    if c < chunks - 1:
                        mixed[k] = part
                        continue
                    _, x, y = place(g, j0 + i)
                    lapse = 1.0 + 0.25 * jnp.tanh(box[0, x + H, y + H][0:1, :])
                    for n in range(chunks):
                        slope = lapse * part[n * ROWS:(n + 1) * ROWS] + smooth_ref[n, k]
                        slope_ref[rows_of(n, k), :] = slope
                        value_ref[rows_of(n, k), :] = box[n, x + H, y + H] + 0.125 * slope
            return 0

        lax.fori_loop(0, groups, step, 0)

    move_z(0)
    send_old(0)
    for c in range(1, chunks):
        move_z(c)
    for c in range(chunks):
        to_x[c].sent()
        to_y[c].sent()
        if c + 1 < chunks:
            send_old(c + 1)
            send_corner(c)
        if c > 0:
            move_xy(c - 1)
            if c + 1 == chunks:
                for n in range(c):
                    send_halos(n, True)
    last = chunks - 1
    send_corner(last)
    move_xy(last)
    send_halos(last, True)
    for c in range(chunks):
        compute(c)

    for c in range(chunks):
        edges[c].sent()
    for c in range(chunks):
        corner_y[c].sent()
        corner_x[c].sent()
        for h in halos[c]:
            h.sent()


def local(fields_now, parent, advect, diffuse, box_shift):
    dims = fields_now.shape
    F, NX, NY, NZ = dims
    flat = (F * NX * NY, NZ)
    chunks = F // ROWS
    groups = NX * NY * SLOT // NZ
    f32 = jnp.float32
    edges = pltpu.VMEM((chunks, groups, ROWS, NZ), f32)
    vmem = pl.BlockSpec(memory_space=pltpu.VMEM)
    slope, value = pl.pallas_call(
        functools.partial(kernel, dims),
        out_shape=[jax.ShapeDtypeStruct(flat, f32)] * 2,
        in_specs=[pl.BlockSpec(memory_space=pltpu.SMEM)] + [vmem] * 4,
        out_specs=[vmem] * 2,
        scratch_shapes=[
            pltpu.VMEM((chunks, NX + 2 * H, NY + 2 * H, ROWS, NZ), f32),
            edges, edges, edges, edges, edges,
            pltpu.VMEM((NX * NY, F, NZ), f32),
            pltpu.VMEM((chunks, NX * NY, ROWS, NZ), f32),
            pltpu.SemaphoreType.DMA((11 * chunks,)),
            pltpu.SemaphoreType.DMA((11 * chunks,)),
        ] + [pltpu.VMEM((NX + W, NY + W, ROWS, NZ), f32)] * chunks,
        compiler_params=pltpu.CompilerParams(
            collective_id=0, has_side_effects=True, vmem_limit_bytes=20 * 2**20
        ),
    )(box_shift, fields_now.reshape(flat), parent.reshape(flat), advect, diffuse)
    return slope.reshape(dims), value.reshape(dims)


def solution(mesh):
    return jax.shard_map(
        local,
        mesh=mesh,
        in_specs=(P(None, "gx", "gy", "gz"), P(None, "gx", "gy", "gz"), P(), P(), P()),
        out_specs=(P(None, "gx", "gy", "gz"), P(None, "gx", "gy", "gz")),
        check_vma=False,
    )
```

```python
import functools

import jax
import jax.numpy as jnp
from jax import lax
from jax.experimental import pallas as pl
from jax.experimental.pallas import tpu as pltpu
from jax.sharding import PartitionSpec as P

MESH = pl.DeviceIdType.MESH
W = 4
H = 3
SLOT = 8
ROWS = 8
AXES = ("gx", "gy", "gz")


def roll(value, by):
    return pltpu.roll(value, by % value.shape[-1], value.ndim - 1)


def kernel(
    dims, shift_hbm, now_hbm, parent_hbm, advect_hbm, diffuse_hbm, slope_ref, value_ref,
    shift_ref, now_ref, parent_ref, advect_ref, diffuse_ref, box, edge, edge_in, rim, rim_up, rim_low, mixed, smooth_ref,
    send_sem, recv_sem, load_sem, *old,
):
    F, NX, NY, NZ = dims
    chunks = F // ROWS
    cells = NX * NY
    slots = NZ // SLOT
    groups = cells // slots
    me = {a: lax.axis_index(a) for a in AXES}
    size = {a: lax.axis_size(a) for a in AXES}
    below = {a: me[a] > 0 for a in AXES}
    above = {a: me[a] < size[a] - 1 for a in AXES}
    sems = iter(range(11 * chunks))

    loads = []
    span = ROWS * cells
    for c in range(chunks):
        part = pl.ds(c * span, span)
        loads.append(pltpu.make_async_copy(now_hbm.at[part], now_ref.at[part], load_sem.at[c]))
    loads += [
        pltpu.make_async_copy(src, dst, load_sem.at[chunks + n])
        for n, (src, dst) in enumerate((
            (shift_hbm, shift_ref), (parent_hbm, parent_ref),
            (advect_hbm, advect_ref), (diffuse_hbm, diffuse_ref),
        ))
    ]
    for n in (0, chunks, *range(1, chunks), *range(chunks + 1, chunks + 4)):
        loads[n].start()

    class Copy:
        def __init__(self, src, dst, axis, by):
            n = next(sems)
            self.sends = below[axis] if by < 0 else above[axis]
            self.gets = above[axis] if by < 0 else below[axis]
            self.copy = pltpu.make_async_remote_copy(
                src_ref=src, dst_ref=dst, send_sem=send_sem.at[n], recv_sem=recv_sem.at[n],
                device_id={axis: me[axis] + by}, device_id_type=MESH,
            )

        def start(self):
            pl.when(self.sends)(self.copy.start)

        def arrived(self):
            pl.when(self.gets)(self.copy.wait_recv)

        def sent(self):
            pl.when(self.sends)(self.copy.wait_send)

    rim_up[...] = jnp.zeros_like(rim_up)
    rim_low[...] = jnp.zeros_like(rim_low)
    blank = jnp.zeros((ROWS, NZ), jnp.float32)

    def clear_x(y, _):
        for c in range(chunks):
            for x in (*range(H), *range(NX + H, NX + 2 * H)):
                box[c, x, y + H] = blank
        return 0

    def clear_y(x, _):
        for c in range(chunks):
            for y in (*range(H), *range(NY + H, NY + 2 * H)):
                box[c, x + H, y] = blank
        return 0

    lax.fori_loop(0, NY, clear_x, 0)
    lax.fori_loop(0, NX, clear_y, 0)

    barrier = pltpu.get_barrier_semaphore()
    count = 0
    for a in AXES:
        for cond, by in ((below[a], -1), (above[a], 1)):
            @pl.when(cond)
            def _(a=a, by=by):
                pl.semaphore_signal(
                    barrier, inc=1, device_id={a: me[a] + by}, device_id_type=MESH
                )
        count = count + jnp.where(me[a] > 0, 1, 0) + jnp.where(me[a] < size[a] - 1, 1, 0)

    lane = lax.broadcasted_iota(jnp.int32, (ROWS, NZ), 1)
    slot_of = ((lane + SLOT // 2) % NZ) // SLOT

    def place(g, j):
        k = g * slots + j
        return k, g * (slots // NY) + j // NY, j % NY

    def rows_of(c, k):
        return pl.ds(c * ROWS * cells + k, ROWS, stride=cells)

    def pack_old(c):
        def step(g, _):
            packed = blank
            for j in range(slots):
                k, _, _ = place(g, j)
                packed = jnp.where(slot_of == j, roll(now_ref[rows_of(c, k), :], SLOT * j), packed)
            edge[c, g] = packed
            return 0

        lax.fori_loop(0, groups, step, 0)

    edges = [Copy(edge.at[c], edge_in.at[c], "gz", -1) for c in range(chunks)]
    for c in range(chunks):
        loads[c].wait()
        pack_old(c)
        if c == 0:
            pl.semaphore_wait(barrier, count)
        edges[c].start()

    X, Y = pl.ds(0, NX), pl.ds(0, NY)
    BX, BY = pl.ds(H, NX), pl.ds(H, NY)
    half = W // 2
    near, far = pl.ds(NX, half), pl.ds(NX + half, half)
    to_x, to_y, corner_y, corner_x, halos = [], [], [], [], []
    for c in range(chunks):
        o, b = old[c], box.at[c]
        to_x.append(Copy(o.at[pl.ds(0, W), Y], o.at[pl.ds(NX, W), Y], "gx", -1))
        to_y.append(Copy(o.at[X, pl.ds(0, W)], o.at[X, pl.ds(NY, W)], "gy", -1))
        corner_y.append(Copy(o.at[near, pl.ds(0, W)], o.at[near, pl.ds(NY, W)], "gy", -1))
        corner_x.append(
            Copy(o.at[pl.ds(half, half), pl.ds(NY, W)], o.at[far, pl.ds(NY, W)], "gx", -1)
        )
        halos.append([
            Copy(b.at[pl.ds(H, H), BY], b.at[pl.ds(NX + H, H), BY], "gx", -1),
            Copy(b.at[pl.ds(NX, H), BY], b.at[pl.ds(0, H), BY], "gx", 1),
            Copy(b.at[BX, pl.ds(H, H)], b.at[BX, pl.ds(NY + H, H)], "gy", -1),
            Copy(b.at[BX, pl.ds(NY, H)], b.at[BX, pl.ds(0, H)], "gy", 1),
            Copy(rim.at[c], rim_up.at[c], "gz", -1),
            Copy(rim.at[c], rim_low.at[c], "gz", 1),
        ])

    loads[chunks].wait()
    move = [shift_ref[d] for d in range(3)]

    def move_z(c):
        edges[c].arrived()

        def step(g, _):
            for j in range(slots):
                k, x, y = place(g, j)
                tail = roll(edge_in[c, g], -SLOT * j)
                row = jnp.where(lane < move[2], tail, now_ref[rows_of(c, k), :])
                old[c][x, y] = pltpu.roll(row, NZ - move[2], 1)
            return 0

        lax.fori_loop(0, groups, step, 0)

    def send_old(c):
        to_x[c].start()
        to_y[c].start()

    def send_corner(c):
        to_x[c].arrived()
        corner_y[c].start()
        to_y[c].arrived()
        corner_x[c].start()

    def send_halos(c, down):
        for n, h in enumerate(halos[c]):
            if (n in (0, 2)) == down:
                h.start()

    in_z = me["gz"] * NZ + lane + move[2] < size["gz"] * NZ

    def move_xy(c):
        corner_y[c].arrived()
        corner_x[c].arrived()

        def step(g, _):
            packed = blank
            for j in range(slots):
                k, x, y = place(g, j)
                in_x = me["gx"] * NX + x + move[0] < size["gx"] * NX
                in_y = me["gy"] * NY + y + move[1] < size["gy"] * NY
                row = jnp.where(
                    in_z & (in_x & in_y),
                    old[c][x + move[0], y + move[1]],
                    parent_ref[rows_of(c, k), :],
                )
                box[c, x + H, y + H] = row
                packed = jnp.where(slot_of == j, roll(row, SLOT * j), packed)
            rim[c, g] = packed
            return 0

        lax.fori_loop(0, groups, step, 0)
        send_halos(c, False)

    def split(value):
        high = value.astype(jnp.bfloat16)
        return high, (value - high.astype(jnp.float32)).astype(jnp.bfloat16)

    def terms(u, at):
        d1, s1 = at(1) - at(-1), at(1) + at(-1)
        d2, s2 = at(2) - at(-2), at(2) + at(-2)
        s3 = at(3) + at(-3)
        first = 8.0 * d1 - d2
        second = 16.0 * s1 - 30.0 * u - s2
        sixth = s3 - 6.0 * s2 + 15.0 * s1 - 20.0 * u
        return first, second, sixth

    def compute(c):
        for h in halos[c]:
            h.arrived()
        fields = slice(c * ROWS, (c + 1) * ROWS)
        mats = [m[a][:, fields] for a in range(3) for m in (advect_ref, diffuse_ref)]
        m_high, m_low = split(jnp.concatenate(mats, axis=1) / 12.0)
        dot = functools.partial(jnp.dot, preferred_element_type=jnp.float32)

        def step(g, _):
            rims = jnp.where(lane % SLOT < SLOT // 2, rim_up[c, g], rim_low[c, g])
            for j0 in range(0, slots, 2):
                columns = []
                for j in (j0, j0 + 1):
                    k, x, y = place(g, j)
                    u = box[c, x + H, y + H]
                    ends = roll(rims, -SLOT * j)
                    z_at = {}
                    for o in range(1, H + 1):
                        z_at[o] = roll(jnp.where(lane < o, ends, u), -o)
                        z_at[-o] = roll(jnp.where(lane >= NZ - o, ends, u), o)
                    fx, sx, x6 = terms(u, lambda o: box[c, x + H + o, y + H])
                    fy, sy, y6 = terms(u, lambda o: box[c, x + H, y + H + o])
                    fz, sz, z6 = terms(u, lambda o: z_at[o])
                    columns.append(jnp.concatenate([fx, sx, fy, sy, fz, sz], axis=0))
                    smooth_ref[c, k] = (x6 + y6 + z6) * (1.0 / 64.0)
                high, low = split(jnp.concatenate(columns, axis=1))
                linear = dot(m_high, high) + (dot(m_low, high) + dot(m_high, low))
                for i in range(2):
                    k = g * slots + j0 + i
                    part = linear[:, i * NZ:(i + 1) * NZ]
                    if c > 0:
                        part = part + mixed[k]
                    if c < chunks - 1:
                        mixed[k] = part
                        continue
                    _, x, y = place(g, j0 + i)
                    lapse = 1.0 + 0.25 * jnp.tanh(box[0, x + H, y + H][0:1, :])
                    for n in range(chunks):
                        slope = lapse * part[n * ROWS:(n + 1) * ROWS] + smooth_ref[n, k]
                        slope_ref[rows_of(n, k), :] = slope
                        value_ref[rows_of(n, k), :] = box[n, x + H, y + H] + 0.125 * slope
            return 0

        lax.fori_loop(0, groups, step, 0)

    move_z(0)
    send_old(0)
    for c in range(1, chunks):
        move_z(c)
    for load in loads[chunks + 1:]:
        load.wait()
    for c in range(chunks):
        to_x[c].sent()
        to_y[c].sent()
        if c + 1 < chunks:
            send_old(c + 1)
            send_corner(c)
        if c > 0:
            move_xy(c - 1)
            if c + 1 == chunks:
                for n in range(c):
                    send_halos(n, True)
    last = chunks - 1
    send_corner(last)
    move_xy(last)
    send_halos(last, True)
    for c in range(chunks):
        compute(c)

    for c in range(chunks):
        edges[c].sent()
    for c in range(chunks):
        corner_y[c].sent()
        corner_x[c].sent()
        for h in halos[c]:
            h.sent()


def local(fields_now, parent, advect, diffuse, box_shift):
    dims = fields_now.shape
    F, NX, NY, NZ = dims
    flat = (F * NX * NY, NZ)
    chunks = F // ROWS
    groups = NX * NY * SLOT // NZ
    f32 = jnp.float32
    edges = pltpu.VMEM((chunks, groups, ROWS, NZ), f32)
    vmem = pl.BlockSpec(memory_space=pltpu.VMEM)
    slope, value = pl.pallas_call(
        functools.partial(kernel, dims),
        out_shape=[jax.ShapeDtypeStruct(flat, f32)] * 2,
        in_specs=[pl.BlockSpec(memory_space=pltpu.HBM)] * 5,
        out_specs=[vmem] * 2,
        scratch_shapes=[
            pltpu.SMEM(box_shift.shape, jnp.int32),
            pltpu.VMEM(flat, f32),
            pltpu.VMEM(flat, f32),
            pltpu.VMEM(advect.shape, f32),
            pltpu.VMEM(diffuse.shape, f32),
            pltpu.VMEM((chunks, NX + 2 * H, NY + 2 * H, ROWS, NZ), f32),
            edges, edges, edges, edges, edges,
            pltpu.VMEM((NX * NY, F, NZ), f32),
            pltpu.VMEM((chunks, NX * NY, ROWS, NZ), f32),
            pltpu.SemaphoreType.DMA((11 * chunks,)),
            pltpu.SemaphoreType.DMA((11 * chunks,)),
            pltpu.SemaphoreType.DMA((chunks + 4,)),
        ] + [pltpu.VMEM((NX + W, NY + W, ROWS, NZ), f32)] * chunks,
        compiler_params=pltpu.CompilerParams(
            collective_id=0, has_side_effects=True
        ),
    )(box_shift, fields_now.reshape(flat), parent.reshape(flat), advect, diffuse)
    return slope.reshape(dims), value.reshape(dims)


def solution(mesh):
    return jax.shard_map(
        local,
        mesh=mesh,
        in_specs=(P(None, "gx", "gy", "gz"), P(None, "gx", "gy", "gz"), P(), P(), P()),
        out_specs=(P(None, "gx", "gy", "gz"), P(None, "gx", "gy", "gz")),
        check_vma=False,
    )
```
